32 devices in a mesh: grp: 2 (over x), dap: 16 (over z, y, core).
Axes of the slice: x: 2, y: 2, z: 4, core: 2. Of those that a mesh axis runs over, the one named last changes fastest.
Arguments:
- homolog_stack_tensor: bfloat16 [64, 64, 256], P(('grp', 'dap')), parts along dimension 0, may hold values from -6.5 to 6.5
- occupancy_indicator: int32 [64, 64], P('grp'), parts along dimension 0, may hold values from 0 to 1, as said below
- chain_existence_flags: int32 [64], P('grp'), parts along dimension 0, may hold values from 0 to 1, as said below
- focus_normal_factor: float32 [256], replicated, may hold values from 0.25 to 1.75
- focus_normal_addend: float32 [256], replicated, may hold values from -3 to 3
- probe_index_weights: bfloat16 [256, 512], replicated, may hold values from -3 to 3
- payload_valve_weights: bfloat16 [256, 512], replicated, may hold values from -0.375 to 0.375
- logistic_valve_addend: float32 [256], replicated, may hold values from -4 to 4
- focus_exit_weights: bfloat16 [256, 256], replicated, may hold values from -0.375 to 0.375
- focus_exit_addend: float32 [256], replicated, may hold values from -3 to 3
- product_mean_layer_stretch: float32 [256], replicated, may hold values from 0.25 to 1.75
- product_mean_layer_shift: float32 [256], replicated, may hold values from -2 to 2
- twin_map_matrix: bfloat16 [256, 64], replicated, may hold values from -0.375 to 0.375
- twin_map_shift: float32 [64], replicated, may hold values from -2 to 2
- couple_map_matrix: bfloat16 [1024, 128], replicated, may hold values from -0.75 to 0.75
- couple_map_shift: float32 [128], replicated, may hold values from -3 to 3
Outputs:
- alignment_after: bfloat16 [64, 64, 256], P('grp', 'dap'), parts along dimension 0
- pair_features_after: bfloat16 [128, 64, 128], P(('grp', 'dap')), parts along dimension 0
The draws below stay inside these ranges and needn't reach their ends.
There are 2 independent parts, one for each index of `grp`. The reference program is written for one: setup_inputs(seed, part) draws one part's arguments, and reference() takes and returns one part's arrays. A program takes and returns all parts, laid end to end along the dimension named above; an argument that names none is the same for every part. Nothing has to cross between parts.
Inputs may be any that keep to these rules, and one draw needn't show every extreme that they name: `chain_existence_flags`: 1 for the first 16 sequences, 0 for the last one. `occupancy_indicator`: every sequence is 0 from some residue on (the last residue always, never more than the last 32); before it sequence 0 is all 1 and the others have gaps.
All inputs are finite; a program needn't handle non-finite values.
Results may differ from the reference program's by a relative error of at most 0.008.
Values may be sent and summed in bfloat16 or wider, within the bound.
A program may use at most 64 MiB of HBM per device.

```python
import jax
import jax.numpy as jnp
from jax import lax

ALIGN_CHANNELS = 256
HEAD_COUNT = 8
HEAD_CHANNELS = 32
OUTER_CHANNELS = 32
PAIR_DIM = 128
SITES_EACH_SLICE = 4
SEQUENCE_COUNT = 32
RESIDUE_COUNT = 64


def draw_homolog_stack_tensor(key, part):
    random_root_key = jax.random.fold_in(jax.random.fold_in(key, 101), 0)
    value_vectors = jax.random.normal(random_root_key, (SEQUENCE_COUNT, RESIDUE_COUNT, ALIGN_CHANNELS), jnp.float32)
    return jnp.clip(value_vectors, -6.5, 6.5).astype(jnp.bfloat16)


def draw_probe_index_weights(key, part):
    query_seed_value, second_seed_value = jax.random.split(jax.random.fold_in(key, 202))
    inner_channel_width = HEAD_COUNT * HEAD_CHANNELS
    square_root_width = jnp.sqrt(jnp.float32(ALIGN_CHANNELS))
    query_rows_all = jnp.clip(jax.random.normal(query_seed_value, (ALIGN_CHANNELS, inner_channel_width), jnp.float32), -6.0, 6.0) / square_root_width
    key_portion = jnp.clip(jax.random.normal(second_seed_value, (ALIGN_CHANNELS, inner_channel_width), jnp.float32), -6.0, 6.0) / square_root_width
    combined = jnp.concatenate([query_rows_all, key_portion], axis=1)
    return jnp.clip(combined, -3.0, 3.0).astype(jnp.bfloat16)


def draw_chain_existence_flags(key, part):
    coin_flips = jax.random.randint(jax.random.fold_in(key, 303), (SEQUENCE_COUNT,), 0, 2)
    position = jnp.arange(SEQUENCE_COUNT, dtype=jnp.int32)
    forced_on = position < SEQUENCE_COUNT // 2
    forced_off = position == SEQUENCE_COUNT - 1
    return jnp.where(forced_on, 1, jnp.where(forced_off, 0, coin_flips)).astype(jnp.int32)


def draw_occupancy_indicator(key, part):
    length_key, gap_key = jax.random.split(jax.random.fold_in(key, 404))
    length = jax.random.randint(length_key, (), RESIDUE_COUNT // 2, RESIDUE_COUNT)
    gap_draw = jax.random.randint(gap_key, (SEQUENCE_COUNT, RESIDUE_COUNT), 0, 8)
    inside = jnp.arange(RESIDUE_COUNT, dtype=jnp.int32)[None, :] < length
    first_row = jnp.arange(SEQUENCE_COUNT, dtype=jnp.int32)[:, None] == 0
    return (inside & ((gap_draw != 0) | first_row)).astype(jnp.int32)


def gaussian(own_key, shape, scale, limit, kind=jnp.bfloat16):
    entries = jax.random.normal(own_key, shape, jnp.float32) * scale
    return jnp.minimum(jnp.maximum(entries, -limit), limit).astype(kind)


def setup_inputs(seed: int = 0, part: int = 0) -> dict:
    key_list = jax.random.split(jax.random.key(seed), 17)
    part_keys = jax.random.split(jax.random.fold_in(key_list[16], part), 17)
    return {
        "homolog_stack_tensor": draw_homolog_stack_tensor(jax.random.fold_in(jax.random.fold_in(key_list[16], part), 71), part),
        "occupancy_indicator": draw_occupancy_indicator(jax.random.fold_in(jax.random.fold_in(key_list[16], part), 71), part),
        "chain_existence_flags": draw_chain_existence_flags(jax.random.fold_in(jax.random.fold_in(key_list[16], part), 71), part),
        "focus_normal_factor": jnp.clip(1.0 + 0.15 * jax.random.normal(key_list[3], (ALIGN_CHANNELS,), jnp.float32), 0.25, 1.75),
        "focus_normal_addend": gaussian(key_list[4], (ALIGN_CHANNELS,), 0.5, 3.0, jnp.float32),
        "probe_index_weights": draw_probe_index_weights(jax.random.fold_in(key_list[16], 71), part),
        "payload_valve_weights": gaussian(key_list[6], (ALIGN_CHANNELS, 2 * HEAD_COUNT * HEAD_CHANNELS), ALIGN_CHANNELS ** -0.5, 0.375),
        "logistic_valve_addend": gaussian(key_list[7], (HEAD_COUNT * HEAD_CHANNELS,), 1.0, 4.0, jnp.float32),
        "focus_exit_weights": gaussian(key_list[8], (HEAD_COUNT * HEAD_CHANNELS, ALIGN_CHANNELS), (HEAD_COUNT * HEAD_CHANNELS) ** -0.5, 0.375),
        "focus_exit_addend": gaussian(key_list[9], (ALIGN_CHANNELS,), 0.5, 3.0, jnp.float32),
        "product_mean_layer_stretch": jnp.clip(1.0 + 0.15 * jax.random.normal(key_list[10], (ALIGN_CHANNELS,), jnp.float32), 0.25, 1.75),
        "product_mean_layer_shift": gaussian(key_list[11], (ALIGN_CHANNELS,), 0.3, 2.0, jnp.float32),
        "twin_map_matrix": gaussian(key_list[12], (ALIGN_CHANNELS, 2 * OUTER_CHANNELS), ALIGN_CHANNELS ** -0.5, 0.375),
        "twin_map_shift": gaussian(key_list[13], (2 * OUTER_CHANNELS,), 0.3, 2.0, jnp.float32),
        "couple_map_matrix": gaussian(key_list[14], (OUTER_CHANNELS * OUTER_CHANNELS, PAIR_DIM), (OUTER_CHANNELS * OUTER_CHANNELS // 16) ** -0.5, 0.75),
        "couple_map_shift": gaussian(key_list[15], (PAIR_DIM,), 0.5, 3.0, jnp.float32),
    }


EPSILON = 1e-05
MASKED = -100000.0

def layer_norm(value_vectors, scale_vec, shift_vec):
    widened = value_vectors.astype(jnp.float32)
    centred = widened - lax.optimization_barrier(jnp.mean(widened, axis=-1, keepdims=True))
    variance = lax.optimization_barrier(jnp.mean(centred * centred, axis=-1, keepdims=True))
    scaled = centred * lax.rsqrt(variance + EPSILON)
    return (scaled * scale_vec.astype(jnp.float32) + shift_vec.astype(jnp.float32)).astype(jnp.bfloat16)

def heed_across_lanes(vertical_pieces, present_mask, focus_normal_factor, focus_normal_addend, probe_index_weights, payload_valve_weights, logistic_valve_addend, focus_exit_weights, focus_exit_addend):
    seq_count, res_count, feature_width = vertical_pieces.shape
    inner_channel_width = HEAD_COUNT * HEAD_CHANNELS
    normed = layer_norm(vertical_pieces, focus_normal_factor, focus_normal_addend).reshape(seq_count * res_count, feature_width)
    query_key = jnp.dot(normed, probe_index_weights, preferred_element_type=jnp.float32)
    value_gate = jnp.dot(normed, payload_valve_weights, preferred_element_type=jnp.float32)
    head_shape = (seq_count, res_count, HEAD_COUNT, HEAD_CHANNELS)
    query_rows_all = (query_key[:, :inner_channel_width] * HEAD_CHANNELS ** (-0.5)).astype(jnp.bfloat16).reshape(head_shape)
    key_rows = query_key[:, inner_channel_width:].astype(jnp.bfloat16).reshape(head_shape)
    value_rows = value_gate[:, :inner_channel_width].astype(jnp.bfloat16).reshape(head_shape)
    gating = jax.nn.sigmoid(value_gate[:, inner_channel_width:] + logistic_valve_addend.astype(jnp.float32))
    scores = jnp.einsum('srhd,trhd->rhst', query_rows_all.astype(jnp.float32), key_rows.astype(jnp.float32))
    allowed = jnp.transpose(present_mask > 0)[:, None, None, :]
    scores = jnp.where(allowed, scores, MASKED)
    exponent = jnp.exp(scores - lax.optimization_barrier(jnp.max(scores, axis=-1, keepdims=True)))
    weights = (exponent / lax.optimization_barrier(jnp.sum(exponent, axis=-1, keepdims=True))).astype(jnp.bfloat16)
    attended = jnp.einsum('rhst,trhd->srhd', weights.astype(jnp.float32), value_rows.astype(jnp.float32))
    gated_rows = (attended.reshape(seq_count * res_count, inner_channel_width) * gating).astype(jnp.bfloat16)
    update = jnp.dot(gated_rows, focus_exit_weights, preferred_element_type=jnp.float32) + focus_exit_addend.astype(jnp.float32)
    return (vertical_pieces.astype(jnp.float32) + update.reshape(seq_count, res_count, feature_width)).astype(jnp.bfloat16)

def project_pairs(revised_tensor, present_mask, product_mean_layer_stretch, product_mean_layer_shift, twin_map_matrix, twin_map_shift):
    seq_count, res_count, feature_width = revised_tensor.shape
    normed = layer_norm(revised_tensor, product_mean_layer_stretch, product_mean_layer_shift).reshape(seq_count * res_count, feature_width)
    projected = jnp.dot(normed, twin_map_matrix, preferred_element_type=jnp.float32) + twin_map_shift.astype(jnp.float32)
    projected = projected.reshape(seq_count, res_count, 2 * OUTER_CHANNELS) * present_mask[:, :, None].astype(jnp.float32)
    projected = projected.astype(jnp.bfloat16)
    return (projected[:, :, :OUTER_CHANNELS], projected[:, :, OUTER_CHANNELS:])

def pair_tile(left_rows, right_cols, live_rows, live_cols, couple_map_matrix, couple_map_shift):
    row_count = left_rows.shape[1]
    col_count = right_cols.shape[1]
    outer_sum = jnp.einsum('sic,sje->ijce', left_rows.astype(jnp.float32), right_cols.astype(jnp.float32))
    counts = jnp.einsum('si,sj->ij', live_rows.astype(jnp.float32), live_cols.astype(jnp.float32))
    mean_terms = (outer_sum.reshape(row_count, col_count, OUTER_CHANNELS * OUTER_CHANNELS) / jnp.maximum(counts, 1.0)[:, :, None]).astype(jnp.bfloat16)
    result = jnp.dot(mean_terms.reshape(row_count * col_count, OUTER_CHANNELS * OUTER_CHANNELS), couple_map_matrix, preferred_element_type=jnp.float32)
    result = result + couple_map_shift.astype(jnp.float32)
    return result.astype(jnp.bfloat16).reshape(row_count, col_count, PAIR_DIM)

def reference(homolog_stack_tensor, occupancy_indicator, chain_existence_flags, focus_normal_factor, focus_normal_addend, probe_index_weights, payload_valve_weights, logistic_valve_addend, focus_exit_weights, focus_exit_addend, product_mean_layer_stretch, product_mean_layer_shift, twin_map_matrix, twin_map_shift, couple_map_matrix, couple_map_shift):
    present_mask = occupancy_indicator * chain_existence_flags[:, None]
    block_count = RESIDUE_COUNT // SITES_EACH_SLICE

    def column_block(block_index):
        opening_index = (block_index * SITES_EACH_SLICE).astype(jnp.int32)
        homolog_owned_block = lax.dynamic_slice_in_dim(homolog_stack_tensor, opening_index, SITES_EACH_SLICE, 1)
        current_fraction = lax.dynamic_slice_in_dim(present_mask, opening_index, SITES_EACH_SLICE, 1)
        revised_tensor = heed_across_lanes(homolog_owned_block, current_fraction, focus_normal_factor, focus_normal_addend, probe_index_weights, payload_valve_weights, logistic_valve_addend, focus_exit_weights, focus_exit_addend)
        left_part, right_part = project_pairs(revised_tensor, current_fraction, product_mean_layer_stretch, product_mean_layer_shift, twin_map_matrix, twin_map_shift)
        return (revised_tensor, left_part, right_part)
    refreshed_blocks, left_blocks, right_blocks = lax.map(column_block, jnp.arange(block_count, dtype=jnp.int32))
    alignment_after = jnp.transpose(refreshed_blocks, (1, 0, 2, 3)).reshape(SEQUENCE_COUNT, RESIDUE_COUNT, ALIGN_CHANNELS)
    left_all = jnp.transpose(left_blocks, (1, 0, 2, 3)).reshape(SEQUENCE_COUNT, RESIDUE_COUNT, OUTER_CHANNELS)
    right_all = jnp.transpose(right_blocks, (1, 0, 2, 3)).reshape(SEQUENCE_COUNT, RESIDUE_COUNT, OUTER_CHANNELS)

    def pair_block(block_index):
        opening_index = (block_index * SITES_EACH_SLICE).astype(jnp.int32)
        rows_left = lax.dynamic_slice_in_dim(left_all, opening_index, SITES_EACH_SLICE, 1)
        rows_live = lax.dynamic_slice_in_dim(present_mask, opening_index, SITES_EACH_SLICE, 1)
        return pair_tile(rows_left, right_all, rows_live, present_mask, couple_map_matrix, couple_map_shift)
    pair_blocks = lax.map(pair_block, jnp.arange(block_count, dtype=jnp.int32))
    pair_features_after = pair_blocks.reshape(RESIDUE_COUNT, RESIDUE_COUNT, PAIR_DIM)
    return (alignment_after, pair_features_after)
```

```python
import functools

import jax
import jax.numpy as jnp
from jax import lax
from jax.experimental import pallas as pl
from jax.experimental.pallas import tpu as pltpu
from jax.sharding import PartitionSpec as P

HEAD_COUNT = 8
HEAD_CHANNELS = 32
OUTER_CHANNELS = 32
PAIR_DIM = 128
EPSILON = 1e-05
MASKED = -100000.0
OTHER = -3.0e38
CHUNK = 128

F32 = jnp.float32
BF16 = jnp.bfloat16
MESH = pl.DeviceIdType.MESH


def iota(shape, dim):
    return lax.broadcasted_iota(jnp.int32, shape, dim)


def dot(a, b):
    return jnp.dot(a, b, preferred_element_type=F32)


def dot_t(a, b):
    return lax.dot_general(a, b, (((1,), (1,)), ((), ())), preferred_element_type=F32)


def layer_norm(x, scale, shift):
    centred = x - jnp.mean(x, axis=-1, keepdims=True)
    variance = jnp.mean(centred * centred, axis=-1, keepdims=True)
    return (centred * lax.rsqrt(variance + EPSILON) * scale + shift).astype(BF16)


def repeat(count, body):
    if count == 1:
        body(0)
    else:
        lax.fori_loop(0, count, lambda i, c: (body(i), c)[1], 0)


def each_peer(n, body):
    if n <= 16:
        for k in range(1, n):
            body(k)
    else:
        lax.fori_loop(1, n, lambda k, c: (body(k), c)[1], 0)


def kernel(
    n,
    x_ref, occ_ref, flag_ref, ng_ref, na_ref, wqk_hbm, wvg_hbm, gb_ref, wo_hbm, ob_ref,
    pg_ref, pa_ref, wt_ref, bt_ref, cm_hbm, cb_ref,
    out_ref, pair_ref,
    send, recv, rsend, rbuf, wqk, wvg, wo, cm, cmf, w2,
    q_s, kb_s, vb_s, g_s, t_s, inv_s, live_s,
    wsem, ssem, rsem, ssem2, rsem2,
):
    me = lax.axis_index("dap")
    own, res, width = x_ref.shape
    local = res // n
    seqs = occ_ref.shape[0]
    tokens = seqs * local
    chunks = tokens // CHUNK
    per = CHUNK // local
    ke = OUTER_CHANNELS * per

    loads = [
        pltpu.make_async_copy(src, dst, wsem.at[i])
        for i, (src, dst) in enumerate(
            ((cm_hbm, cm), (wqk_hbm, wqk), (wvg_hbm, wvg), (wo_hbm, wo))
        )
    ]
    for load in loads:
        load.start()

    barrier = pltpu.get_barrier_semaphore()

    def greet(k):
        pl.semaphore_signal(
            barrier, inc=1, device_id={"dap": lax.rem(me + k, n)}, device_id_type=MESH
        )

    each_peer(n, greet)

    x32 = x_ref[...].astype(F32)
    for p in range(n):
        rows = [x32[s, local * p : local * (p + 1)] for s in range(own)]
        send[p] = jnp.concatenate(rows, axis=0).astype(BF16)
    recv[me] = send[me]

    pl.semaphore_wait(barrier, n - 1)

    def post(k):
        peer = lax.rem(me + k, n)
        pltpu.make_async_remote_copy(
            src_ref=send.at[peer],
            dst_ref=recv.at[me],
            send_sem=ssem,
            recv_sem=rsem,
            device_id={"dap": peer},
            device_id_type=MESH,
        ).start()

    each_peer(n, post)

    occ = occ_ref[...].astype(F32)
    flag = flag_ref[...].astype(F32)
    pick = (iota((8, res), 1) == me * local + iota((8, res), 0)).astype(F32)
    pick = jnp.where(iota((8, res), 0) < local, pick, 0.0)
    live_rs = dot_t(pick, occ) * flag
    owner = (iota((seqs, tokens), 0) == iota((seqs, tokens), 1) // local).astype(F32)
    live_rt = dot(live_rs, owner)
    same = iota((8, tokens), 0) == lax.rem(iota((8, tokens), 1), local)
    live_row = jnp.sum(jnp.where(same, live_rt, 0.0), axis=0, keepdims=True)
    counts = dot(live_rs, occ)
    eye = (iota((res, res), 0) == iota((res, res), 1)).astype(F32)
    counts_t = lax.dot_general(
        eye, counts, (((1,), (1,)), ((), ())),
        precision=lax.Precision.HIGHEST, preferred_element_type=F32,
    )
    inv_s[...] = 1.0 / jnp.maximum(counts_t, 1.0)

    def live_column(ch):
        token = iota((CHUNK, seqs), 0)
        mine = (token // local + ch * per == iota((CHUNK, seqs), 1)).astype(F32) * flag
        spread = dot(mine, occ)
        here = iota((CHUNK, res), 1) == me * local + lax.rem(iota((CHUNK, res), 0), local)
        live_s[pl.ds(ch * CHUNK, CHUNK), :] = jnp.sum(
            jnp.where(here, spread, 0.0), axis=1, keepdims=True
        )

    repeat(chunks, live_column)

    loads[0].wait()
    cmf[...] = cm[...].astype(F32)
    for e in range(OUTER_CHANNELS):
        w2[0:OUTER_CHANNELS, e * PAIR_DIM : (e + 1) * PAIR_DIM] = cmf[
            pl.ds(e, OUTER_CHANNELS, stride=OUTER_CHANNELS), :
        ].astype(BF16)
    w2[OUTER_CHANNELS:, :] = jnp.zeros((OUTER_CHANNELS, OUTER_CHANNELS * PAIR_DIM), BF16)

    spread_e = (
        iota((2 * OUTER_CHANNELS, ke), 0) == OUTER_CHANNELS + iota((2 * OUTER_CHANNELS, ke), 1) // per
    ).astype(BF16)
    own_seq = iota((CHUNK, ke), 0) // local == lax.rem(iota((CHUNK, ke), 1), per)
    sel = (iota((8, CHUNK), 0) == lax.rem(iota((8, CHUNK), 1), local)).astype(BF16)
    perm_row = iota((CHUNK, CHUNK), 0)
    perm = (
        iota((CHUNK, CHUNK), 1) == lax.rem(perm_row, per) * local + perm_row // per
    ).astype(BF16)
    lane_head = iota((CHUNK, width), 1) // HEAD_CHANNELS

    for load in loads[1:]:
        load.wait()
    pltpu.make_async_copy(recv.at[pl.ds(0, n - 1)], recv.at[pl.ds(0, n - 1)], rsem).wait()

    block = own * local
    blocks = CHUNK // block

    def token_rows(ch):
        return recv[pl.ds(ch * blocks, blocks)].astype(F32).reshape(CHUNK, width)

    def project(ch):
        normed = layer_norm(token_rows(ch), ng_ref[...], na_ref[...])
        qk = dot(normed, wqk[...])
        vg = dot(normed, wvg[...])
        at = pl.ds(ch * CHUNK, CHUNK)
        q_s[at, :] = (qk[:, :width] * HEAD_CHANNELS**-0.5).astype(BF16)
        k = qk[:, width:].astype(BF16)
        v = vg[:, :width].astype(BF16)
        zero = jnp.zeros_like(k)
        one = jnp.ones_like(k)
        for h in range(HEAD_COUNT):
            row = pl.ds(h * tokens + ch * CHUNK, CHUNK)
            kb_s[row, :] = jnp.where(lane_head == h, k, zero)
            vb_s[row, 0:width] = jnp.where(lane_head == h, v, zero)
            vb_s[row, width:] = jnp.where(lane_head == h, one, zero)
        g_s[at, :] = jax.nn.sigmoid(vg[:, width:] + gb_ref[...])

    repeat(chunks, project)

    def attend(ch):
        at = pl.ds(ch * CHUNK, CHUNK)
        q = q_s[at, :]
        alive = live_row > 0.0
        mate = lax.rem(iota((CHUNK, tokens), 0), local) == lax.rem(iota((CHUNK, tokens), 1), local)
        probs = []
        for h in range(HEAD_COUNT):
            scores = dot_t(q, kb_s[h * tokens : (h + 1) * tokens, :])
            scores = jnp.where(mate, jnp.where(alive, scores, MASKED), OTHER)
            probs.append(
                jnp.exp(scores - jnp.max(scores, axis=-1, keepdims=True)).astype(BF16)
            )
        both = dot(jnp.concatenate(probs, axis=1), vb_s[...])
        attended = both[:, :width] / both[:, width:]
        gated = (attended * g_s[at, :]).astype(BF16)
        update = dot(gated, wo[...]) + ob_ref[...]
        after = token_rows(ch) + update
        revised = after.astype(BF16)
        out_ref[pl.ds(ch * per, per)] = after.reshape(per, local, width).astype(BF16)
        normed = layer_norm(revised.astype(F32), pg_ref[...], pa_ref[...])
        projected = (dot(normed, wt_ref[...]) + bt_ref[...]) * live_s[at, :]
        projected = projected.astype(BF16)
        wide = jnp.where(own_seq, dot(projected, spread_e), 0.0).astype(BF16)
        mine = dot(sel, wide)[:local].astype(BF16)
        if chunks == 1:
            rsend[...] = mine
        else:
            rsend[:, pl.ds(pl.multiple_of(ch * ke, ke), ke)] = mine
        if chunks == 1:
            post_right()
        left = dot(perm, projected).astype(BF16)
        for e in range(OUTER_CHANNELS):
            part = dot(left, w2[:, e * PAIR_DIM : (e + 1) * PAIR_DIM]).astype(BF16)
            for i in range(local):
                t_s[ch, e * per : (e + 1) * per, i * PAIR_DIM : (i + 1) * PAIR_DIM] = part[
                    i * per : (i + 1) * per
                ]

    def post_right():
        rbuf[me] = rsend[...]

        def post(k):
            pltpu.make_async_remote_copy(
                src_ref=rsend,
                dst_ref=rbuf.at[me],
                send_sem=ssem2,
                recv_sem=rsem2,
                device_id={"dap": lax.rem(me + k, n)},
                device_id_type=MESH,
            ).start()

        each_peer(n, post)

    repeat(chunks, attend)
    if chunks > 1:
        post_right()

    pltpu.make_async_copy(rbuf.at[pl.ds(0, n - 1)], rbuf.at[pl.ds(0, n - 1)], rsem2).wait()

    total = None
    for ch in range(chunks):
        right = rbuf[:, :, ch * ke : (ch + 1) * ke].astype(F32).reshape(res, ke).astype(BF16)
        part = dot(right, t_s[ch])
        total = part if total is None else total + part
    inv = inv_s[...]
    for i in range(local):
        pair_ref[i] = (
            total[:, i * PAIR_DIM : (i + 1) * PAIR_DIM] * inv[:, i : i + 1] + cb_ref[...]
        ).astype(BF16)

    pltpu.make_async_copy(send.at[pl.ds(0, n - 1)], send.at[pl.ds(0, n - 1)], ssem).wait()
    pltpu.make_async_copy(rbuf.at[pl.ds(0, n - 1)], rbuf.at[pl.ds(0, n - 1)], ssem2).wait()


def shards(n, *args):
    x, occ, flag, ng, na, wqk, wvg, gb, wo, ob, pg, pa, wt, bt, cm, cb = args
    own, res, width = x.shape
    local = res // n
    seqs = occ.shape[0]
    tokens = seqs * local
    chunks = tokens // CHUNK
    ke = OUTER_CHANNELS * (CHUNK // local)
    row = lambda v: v.reshape(1, -1)
    vm = pl.BlockSpec(memory_space=pltpu.VMEM)
    hbm = pl.BlockSpec(memory_space=pl.ANY)
    return pl.pallas_call(
        functools.partial(kernel, n),
        out_shape=(
            jax.ShapeDtypeStruct((seqs, local, width), BF16),
            jax.ShapeDtypeStruct((local, res, PAIR_DIM), BF16),
        ),
        in_specs=[vm, vm, vm, vm, vm, hbm, hbm, vm, hbm, vm, vm, vm, vm, vm, hbm, vm],
        out_specs=(vm, vm),
        scratch_shapes=[
            pltpu.VMEM((n, own * local, width), BF16),
            pltpu.VMEM((n, own * local, width), BF16),
            pltpu.VMEM((local, chunks * ke), BF16),
            pltpu.VMEM((n, local, chunks * ke), BF16),
            pltpu.VMEM(wqk.shape, BF16),
            pltpu.VMEM(wvg.shape, BF16),
            pltpu.VMEM(wo.shape, BF16),
            pltpu.VMEM(cm.shape, BF16),
            pltpu.VMEM(cm.shape, F32),
            pltpu.VMEM((2 * OUTER_CHANNELS, OUTER_CHANNELS * PAIR_DIM), BF16),
            pltpu.VMEM((tokens, width), BF16),
            pltpu.VMEM((HEAD_COUNT * tokens, width), BF16),
            pltpu.VMEM((HEAD_COUNT * tokens, 2 * width), BF16),
            pltpu.VMEM((tokens, width), F32),
            pltpu.VMEM((chunks, ke, local * PAIR_DIM), BF16),
            pltpu.VMEM((res, 8), F32),
            pltpu.VMEM((tokens, 1), F32),
            pltpu.SemaphoreType.DMA((4,)),
            pltpu.SemaphoreType.DMA,
            pltpu.SemaphoreType.DMA,
            pltpu.SemaphoreType.DMA,
            pltpu.SemaphoreType.DMA,
        ],
        compiler_params=pltpu.CompilerParams(
            collective_id=0, has_side_effects=True, vmem_limit_bytes=60 * 1024 * 1024
        ),
        name="evoformer",
    )(x, occ, row(flag), row(ng), row(na), wqk, wvg, row(gb), wo, row(ob),
      row(pg), row(pa), wt, row(bt), cm, row(cb))


def solution(mesh):
    in_specs = (P(("grp", "dap"), None, None), P("grp", None), P("grp")) + (P(),) * 13
    out_specs = (P("grp", "dap", None), P(("grp", "dap"), None, None))
    return jax.shard_map(
        functools.partial(shards, mesh.shape["dap"]),
        mesh=mesh, in_specs=in_specs, out_specs=out_specs, check_vma=False,
    )
```

```python
import functools

import jax
import jax.numpy as jnp
from jax import lax
from jax.experimental import pallas as pl
from jax.experimental.pallas import tpu as pltpu
from jax.sharding import PartitionSpec as P

HEAD_COUNT = 8
HEAD_CHANNELS = 32
OUTER_CHANNELS = 32
PAIR_DIM = 128
EPSILON = 1e-05
MASKED = -100000.0
OTHER = -3.0e38
CHUNK = 128

F32 = jnp.float32
BF16 = jnp.bfloat16
MESH = pl.DeviceIdType.MESH


def iota(shape, dim):
    return lax.broadcasted_iota(jnp.int32, shape, dim)


def dot(a, b):
    return jnp.dot(a, b, preferred_element_type=F32)


def dot_t(a, b):
    return lax.dot_general(a, b, (((1,), (1,)), ((), ())), preferred_element_type=F32)


def layer_norm(x, scale, shift):
    centred = x - jnp.mean(x, axis=-1, keepdims=True)
    variance = jnp.mean(centred * centred, axis=-1, keepdims=True)
    return (centred * lax.rsqrt(variance + EPSILON) * scale + shift).astype(BF16)


def repeat(count, body):
    if count == 1:
        body(0)
    else:
        lax.fori_loop(0, count, lambda i, c: (body(i), c)[1], 0)


def each_peer(n, body):
    if n <= 16:
        for k in range(1, n):
            body(k)
    else:
        lax.fori_loop(1, n, lambda k, c: (body(k), c)[1], 0)


def kernel(
    n,
    x_ref, occ_ref, flag_ref, ng_ref, na_ref, wqk_hbm, wvg_hbm, gb_ref, wo_hbm, ob_ref,
    pg_ref, pa_ref, wt_ref, bt_ref, cm_hbm, cb_ref,
    out_ref, pair_ref,
    send, recv, rsend, rbuf, wqk, wvg, wo, cm, cmf, w2,
    q_s, kb_s, vb_s, g_s, t_s, inv_s, live_s,
    wsem, ssem, rsem, ssem2, rsem2,
):
    me = lax.axis_index("dap")
    own, res, width = x_ref.shape
    local = res // n
    seqs = occ_ref.shape[0]
    tokens = seqs * local
    chunks = tokens // CHUNK
    per = CHUNK // local
    ke = OUTER_CHANNELS * per

    loads = [
        pltpu.make_async_copy(src, dst, wsem.at[i])
        for i, (src, dst) in enumerate(
            ((cm_hbm, cm), (wqk_hbm, wqk), (wvg_hbm, wvg), (wo_hbm, wo))
        )
    ]
    for load in loads:
        load.start()

    barrier = pltpu.get_barrier_semaphore()

    def greet(k):
        pl.semaphore_signal(
            barrier, inc=1, device_id={"dap": lax.rem(me + k, n)}, device_id_type=MESH
        )

    each_peer(n, greet)

    x32 = x_ref[...].astype(F32)
    for p in range(n):
        rows = [x32[s, local * p : local * (p + 1)] for s in range(own)]
        send[p] = jnp.concatenate(rows, axis=0).astype(BF16)
    recv[me] = send[me]

    pl.semaphore_wait(barrier, n - 1)

    def post(k):
        peer = lax.rem(me + k, n)
        pltpu.make_async_remote_copy(
            src_ref=send.at[peer],
            dst_ref=recv.at[me],
            send_sem=ssem,
            recv_sem=rsem,
            device_id={"dap": peer},
            device_id_type=MESH,
        ).start()

    each_peer(n, post)

    occ = occ_ref[...].astype(F32)
    flag = flag_ref[...].astype(F32)
    pick = (iota((8, res), 1) == me * local + iota((8, res), 0)).astype(F32)
    pick = jnp.where(iota((8, res), 0) < local, pick, 0.0)
    live_rs = dot_t(pick, occ) * flag
    owner = (iota((seqs, tokens), 0) == iota((seqs, tokens), 1) // local).astype(F32)
    live_rt = dot(live_rs, owner)
    same = iota((8, tokens), 0) == lax.rem(iota((8, tokens), 1), local)
    live_row = jnp.sum(jnp.where(same, live_rt, 0.0), axis=0, keepdims=True)
    counts = dot(live_rs, occ)
    eye = (iota((res, res), 0) == iota((res, res), 1)).astype(F32)
    counts_t = lax.dot_general(
        eye, counts, (((1,), (1,)), ((), ())),
        precision=lax.Precision.HIGHEST, preferred_element_type=F32,
    )
    inv_s[...] = 1.0 / jnp.maximum(counts_t, 1.0)

    def live_column(ch):
        token = iota((CHUNK, seqs), 0)
        mine = (token // local + ch * per == iota((CHUNK, seqs), 1)).astype(F32) * flag
        spread = dot(mine, occ)
        here = iota((CHUNK, res), 1) == me * local + lax.rem(iota((CHUNK, res), 0), local)
        live_s[pl.ds(ch * CHUNK, CHUNK), :] = jnp.sum(
            jnp.where(here, spread, 0.0), axis=1, keepdims=True
        )

    repeat(chunks, live_column)

    loads[0].wait()
    cmf[...] = cm[...].astype(F32)
    for e in range(OUTER_CHANNELS):
        w2[0:OUTER_CHANNELS, e * PAIR_DIM : (e + 1) * PAIR_DIM] = cmf[
            pl.ds(e, OUTER_CHANNELS, stride=OUTER_CHANNELS), :
        ].astype(BF16)
    w2[OUTER_CHANNELS:, :] = jnp.zeros((OUTER_CHANNELS, OUTER_CHANNELS * PAIR_DIM), BF16)

    spread_e = (
        iota((2 * OUTER_CHANNELS, ke), 0) == OUTER_CHANNELS + iota((2 * OUTER_CHANNELS, ke), 1) // per
    ).astype(BF16)
    own_seq = iota((CHUNK, ke), 0) // local == lax.rem(iota((CHUNK, ke), 1), per)
    sel = (iota((8, CHUNK), 0) == lax.rem(iota((8, CHUNK), 1), local)).astype(BF16)
    perm_row = iota((CHUNK, CHUNK), 0)
    perm = (
        iota((CHUNK, CHUNK), 1) == lax.rem(perm_row, per) * local + perm_row // per
    ).astype(BF16)
    lane_head = iota((CHUNK, width), 1) // HEAD_CHANNELS

    for load in loads[1:]:
        load.wait()
    pltpu.make_async_copy(recv.at[pl.ds(0, n - 1)], recv.at[pl.ds(0, n - 1)], rsem).wait()

    block = own * local
    blocks = CHUNK // block

    def token_rows(ch):
        return recv[pl.ds(ch * blocks, blocks)].astype(F32).reshape(CHUNK, width)

    def project(ch):
        normed = layer_norm(token_rows(ch), ng_ref[...], na_ref[...])
        qk = dot(normed, wqk[...])
        vg = dot(normed, wvg[...])
        at = pl.ds(ch * CHUNK, CHUNK)
        q_s[at, :] = (qk[:, :width] * HEAD_CHANNELS**-0.5).astype(BF16)
        k = qk[:, width:].astype(BF16)
        v = vg[:, :width].astype(BF16)
        zero = jnp.zeros_like(k)
        one = jnp.ones_like(k)
        for h in range(HEAD_COUNT):
            row = pl.ds(h * tokens + ch * CHUNK, CHUNK)
            kb_s[row, :] = jnp.where(lane_head == h, k, zero)
            vb_s[row, 0:width] = jnp.where(lane_head == h, v, zero)
            vb_s[row, width:] = jnp.where(lane_head == h, one, zero)
        g_s[at, :] = jax.nn.sigmoid(vg[:, width:] + gb_ref[...])

    repeat(chunks, project)

    def attend(ch):
        at = pl.ds(ch * CHUNK, CHUNK)
        q = q_s[at, :]
        alive = live_row > 0.0
        mate = lax.rem(iota((CHUNK, tokens), 0), local) == lax.rem(iota((CHUNK, tokens), 1), local)
        probs = []
        for h in range(HEAD_COUNT):
            scores = dot_t(q, kb_s[h * tokens : (h + 1) * tokens, :])
            scores = jnp.where(mate, jnp.where(alive, scores, MASKED), OTHER)
            probs.append(
                jnp.exp(scores - jnp.max(scores, axis=-1, keepdims=True)).astype(BF16)
            )
        both = dot(jnp.concatenate(probs, axis=1), vb_s[...])
        attended = both[:, :width] / both[:, width:]
        gated = (attended * g_s[at, :]).astype(BF16)
        update = dot(gated, wo[...]) + ob_ref[...]
        after = token_rows(ch) + update
        revised = after.astype(BF16)
        out_ref[pl.ds(ch * per, per)] = after.reshape(per, local, width).astype(BF16)
        normed = layer_norm(revised.astype(F32), pg_ref[...], pa_ref[...])
        projected = (dot_t(normed, wt_ref[...]) + bt_ref[...]) * live_s[at, :]
        projected = projected.astype(BF16)
        wide = jnp.where(own_seq, dot(projected, spread_e), 0.0).astype(BF16)
        mine = dot(sel, wide)[:local].astype(BF16)
        if chunks == 1:
            rsend[...] = mine
        else:
            rsend[:, pl.ds(pl.multiple_of(ch * ke, ke), ke)] = mine
        if chunks == 1:
            post_right()
        left = dot(perm, projected).astype(BF16)
        for e in range(OUTER_CHANNELS):
            part = dot(left, w2[:, e * PAIR_DIM : (e + 1) * PAIR_DIM]).astype(BF16)
            for i in range(local):
                t_s[ch, e * per : (e + 1) * per, i * PAIR_DIM : (i + 1) * PAIR_DIM] = part[
                    i * per : (i + 1) * per
                ]

    def post_right():
        rbuf[me] = rsend[...]

        def post(k):
            pltpu.make_async_remote_copy(
                src_ref=rsend,
                dst_ref=rbuf.at[me],
                send_sem=ssem2,
                recv_sem=rsem2,
                device_id={"dap": lax.rem(me + k, n)},
                device_id_type=MESH,
            ).start()

        each_peer(n, post)

    repeat(chunks, attend)
    if chunks > 1:
        post_right()

    pltpu.make_async_copy(rbuf.at[pl.ds(0, n - 1)], rbuf.at[pl.ds(0, n - 1)], rsem2).wait()

    total = None
    for ch in range(chunks):
        right = rbuf[:, :, ch * ke : (ch + 1) * ke].astype(F32).reshape(res, ke).astype(BF16)
        part = dot(right, t_s[ch])
        total = part if total is None else total + part
    inv = inv_s[...]
    for i in range(local):
        pair_ref[i] = (
            total[:, i * PAIR_DIM : (i + 1) * PAIR_DIM] * inv[:, i : i + 1] + cb_ref[...]
        ).astype(BF16)

    pltpu.make_async_copy(send.at[pl.ds(0, n - 1)], send.at[pl.ds(0, n - 1)], ssem).wait()
    pltpu.make_async_copy(rbuf.at[pl.ds(0, n - 1)], rbuf.at[pl.ds(0, n - 1)], ssem2).wait()


def shards(n, *args):
    x, occ, flag, ng, na, wqk, wvg, gb, wo, ob, pg, pa, wt, bt, cm, cb = args
    own, res, width = x.shape
    local = res // n
    seqs = occ.shape[0]
    tokens = seqs * local
    chunks = tokens // CHUNK
    ke = OUTER_CHANNELS * (CHUNK // local)
    row = lambda v: v.reshape(1, -1)
    vm = pl.BlockSpec(memory_space=pltpu.VMEM)
    hbm = pl.BlockSpec(memory_space=pl.ANY)
    return pl.pallas_call(
        functools.partial(kernel, n),
        out_shape=(
            jax.ShapeDtypeStruct((seqs, local, width), BF16),
            jax.ShapeDtypeStruct((local, res, PAIR_DIM), BF16),
        ),
        in_specs=[vm, vm, vm, vm, vm, hbm, hbm, vm, hbm, vm, vm, vm, vm, vm, hbm, vm],
        out_specs=(vm, vm),
        scratch_shapes=[
            pltpu.VMEM((n, own * local, width), BF16),
            pltpu.VMEM((n, own * local, width), BF16),
            pltpu.VMEM((local, chunks * ke), BF16),
            pltpu.VMEM((n, local, chunks * ke), BF16),
            pltpu.VMEM(wqk.shape, BF16),
            pltpu.VMEM(wvg.shape, BF16),
            pltpu.VMEM(wo.shape, BF16),
            pltpu.VMEM(cm.shape, BF16),
            pltpu.VMEM(cm.shape, F32),
            pltpu.VMEM((2 * OUTER_CHANNELS, OUTER_CHANNELS * PAIR_DIM), BF16),
            pltpu.VMEM((tokens, width), BF16),
            pltpu.VMEM((HEAD_COUNT * tokens, width), BF16),
            pltpu.VMEM((HEAD_COUNT * tokens, 2 * width), BF16),
            pltpu.VMEM((tokens, width), F32),
            pltpu.VMEM((chunks, ke, local * PAIR_DIM), BF16),
            pltpu.VMEM((res, 8), F32),
            pltpu.VMEM((tokens, 1), F32),
            pltpu.SemaphoreType.DMA((4,)),
            pltpu.SemaphoreType.DMA,
            pltpu.SemaphoreType.DMA,
            pltpu.SemaphoreType.DMA,
            pltpu.SemaphoreType.DMA,
        ],
        compiler_params=pltpu.CompilerParams(
            collective_id=0, has_side_effects=True, vmem_limit_bytes=60 * 1024 * 1024
        ),
        name="evoformer",
    )(x, occ, row(flag), row(ng), row(na), wqk, wvg, row(gb), wo, row(ob),
      row(pg), row(pa), wt.T, row(bt), cm, row(cb))


def solution(mesh):
    in_specs = (P(("grp", "dap"), None, None), P("grp", None), P("grp")) + (P(),) * 13
    out_specs = (P("grp", "dap", None), P(("grp", "dap"), None, None))
    return jax.shard_map(
        functools.partial(shards, mesh.shape["dap"]),
        mesh=mesh, in_specs=in_specs, out_specs=out_specs, check_vma=False,
    )
```

```python
import functools

import jax
import jax.numpy as jnp
from jax import lax
from jax.experimental import pallas as pl
from jax.experimental.pallas import tpu as pltpu
from jax.sharding import PartitionSpec as P

HEAD_COUNT = 8
HEAD_CHANNELS = 32
OUTER_CHANNELS = 32
PAIR_DIM = 128
EPSILON = 1e-05
MASKED = -100000.0
OTHER = -3.0e38
CHUNK = 128

F32 = jnp.float32
BF16 = jnp.bfloat16
MESH = pl.DeviceIdType.MESH


def iota(shape, dim):
    return lax.broadcasted_iota(jnp.int32, shape, dim)


def dot(a, b):
    return jnp.dot(a, b, preferred_element_type=F32)


def dot_t(a, b):
    return lax.dot_general(a, b, (((1,), (1,)), ((), ())), preferred_element_type=F32)


def layer_norm(x, scale, shift):
    centred = x - jnp.mean(x, axis=-1, keepdims=True)
    variance = jnp.mean(centred * centred, axis=-1, keepdims=True)
    return (centred * lax.rsqrt(variance + EPSILON) * scale + shift).astype(BF16)


def repeat(count, body):
    if count == 1:
        body(0)
    else:
        lax.fori_loop(0, count, lambda i, c: (body(i), c)[1], 0)


def each_peer(n, body):
    if n <= 16:
        for k in range(1, n):
            body(k)
    else:
        lax.fori_loop(1, n, lambda k, c: (body(k), c)[1], 0)


def kernel(
    n,
    x_hbm, occ_hbm, flag_hbm, ng_hbm, na_hbm, wqk_hbm, wvg_hbm, gb_hbm, wo_hbm, ob_hbm,
    pg_hbm, pa_hbm, wt_hbm, bt_hbm, cm_hbm, cb_hbm,
    out_hbm, pair_hbm,
    send, recv, rsend, rbuf, cmf, w2,
    q_s, kb_s, vb_s, g_s, t_s, inv_s, live_s,
    x_ref, occ_ref, flag_ref, ng_ref, na_ref, wqk, wvg, gb_ref, wo, ob_ref,
    pg_ref, pa_ref, wt_ref, bt_ref, cm, cb_ref,
    out_ref, pair_ref,
    wsem, osem, ssem, rsem, ssem2, rsem2,
):
    me = lax.axis_index("dap")
    own, res, width = x_hbm.shape
    local = res // n
    seqs = occ_hbm.shape[0]
    tokens = seqs * local
    chunks = tokens // CHUNK
    per = CHUNK // local
    ke = OUTER_CHANNELS * per

    sources = (
        x_hbm, occ_hbm, flag_hbm, cm_hbm, ng_hbm, na_hbm, wqk_hbm, wvg_hbm, gb_hbm, wo_hbm,
        ob_hbm, pg_hbm, pa_hbm, wt_hbm, bt_hbm, cb_hbm,
    )
    targets = (
        x_ref, occ_ref, flag_ref, cm, ng_ref, na_ref, wqk, wvg, gb_ref, wo,
        ob_ref, pg_ref, pa_ref, wt_ref, bt_ref, cb_ref,
    )
    loads = [
        pltpu.make_async_copy(src, dst, wsem.at[i])
        for i, (src, dst) in enumerate(zip(sources, targets))
    ]
    loads[0].start()
    barrier = pltpu.get_barrier_semaphore()

    def greet(k):
        pl.semaphore_signal(
            barrier, inc=1, device_id={"dap": lax.rem(me + k, n)}, device_id_type=MESH
        )

    each_peer(n, greet)
    for load in loads[1:]:
        load.start()
    loads[0].wait()

    x32 = x_ref[...].astype(F32)
    for p in range(n):
        rows = [x32[s, local * p : local * (p + 1)] for s in range(own)]
        send[p] = jnp.concatenate(rows, axis=0).astype(BF16)
    recv[me] = send[me]

    pl.semaphore_wait(barrier, n - 1)

    def post(k):
        peer = lax.rem(me + k, n)
        pltpu.make_async_remote_copy(
            src_ref=send.at[peer],
            dst_ref=recv.at[me],
            send_sem=ssem,
            recv_sem=rsem,
            device_id={"dap": peer},
            device_id_type=MESH,
        ).start()

    each_peer(n, post)

    loads[1].wait()
    loads[2].wait()
    occ = occ_ref[...].astype(F32)
    flag = flag_ref[...].astype(F32)
    pick = (iota((8, res), 1) == me * local + iota((8, res), 0)).astype(F32)
    pick = jnp.where(iota((8, res), 0) < local, pick, 0.0)
    live_rs = dot_t(pick, occ) * flag
    owner = (iota((seqs, tokens), 0) == iota((seqs, tokens), 1) // local).astype(F32)
    live_rt = dot(live_rs, owner)
    same = iota((8, tokens), 0) == lax.rem(iota((8, tokens), 1), local)
    live_row = jnp.sum(jnp.where(same, live_rt, 0.0), axis=0, keepdims=True)
    counts = dot(live_rs, occ)
    eye = (iota((res, res), 0) == iota((res, res), 1)).astype(F32)
    counts_t = lax.dot_general(
        eye, counts, (((1,), (1,)), ((), ())),
        precision=lax.Precision.HIGHEST, preferred_element_type=F32,
    )
    inv_s[...] = 1.0 / jnp.maximum(counts_t, 1.0)

    def live_column(ch):
        token = iota((CHUNK, seqs), 0)
        mine = (token // local + ch * per == iota((CHUNK, seqs), 1)).astype(F32) * flag
        spread = dot(mine, occ)
        here = iota((CHUNK, res), 1) == me * local + lax.rem(iota((CHUNK, res), 0), local)
        live_s[pl.ds(ch * CHUNK, CHUNK), :] = jnp.sum(
            jnp.where(here, spread, 0.0), axis=1, keepdims=True
        )

    repeat(chunks, live_column)

    loads[3].wait()
    cmf[...] = cm[...].astype(F32)
    for e in range(OUTER_CHANNELS):
        w2[0:OUTER_CHANNELS, e * PAIR_DIM : (e + 1) * PAIR_DIM] = cmf[
            pl.ds(e, OUTER_CHANNELS, stride=OUTER_CHANNELS), :
        ].astype(BF16)
    w2[OUTER_CHANNELS:, :] = jnp.zeros((OUTER_CHANNELS, OUTER_CHANNELS * PAIR_DIM), BF16)

    spread_e = (
        iota((2 * OUTER_CHANNELS, ke), 0) == OUTER_CHANNELS + iota((2 * OUTER_CHANNELS, ke), 1) // per
    ).astype(BF16)
    own_seq = iota((CHUNK, ke), 0) // local == lax.rem(iota((CHUNK, ke), 1), per)
    sel = (iota((8, CHUNK), 0) == lax.rem(iota((8, CHUNK), 1), local)).astype(BF16)
    perm_row = iota((CHUNK, CHUNK), 0)
    perm = (
        iota((CHUNK, CHUNK), 1) == lax.rem(perm_row, per) * local + perm_row // per
    ).astype(BF16)
    lane_head = iota((CHUNK, width), 1) // HEAD_CHANNELS

    for load in loads[4:]:
        load.wait()
    pltpu.make_async_copy(recv.at[pl.ds(0, n - 1)], recv.at[pl.ds(0, n - 1)], rsem).wait()

    block = own * local
    blocks = CHUNK // block

    def token_rows(ch):
        return recv[pl.ds(ch * blocks, blocks)].astype(F32).reshape(CHUNK, width)

    def project(ch):
        normed = layer_norm(token_rows(ch), ng_ref[...], na_ref[...])
        qk = dot(normed, wqk[...])
        vg = dot(normed, wvg[...])
        at = pl.ds(ch * CHUNK, CHUNK)
        q_s[at, :] = (qk[:, :width] * HEAD_CHANNELS**-0.5).astype(BF16)
        k = qk[:, width:].astype(BF16)
        v = vg[:, :width].astype(BF16)
        zero = jnp.zeros_like(k)
        one = jnp.ones_like(k)
        for h in range(HEAD_COUNT):
            row = pl.ds(h * tokens + ch * CHUNK, CHUNK)
            kb_s[row, :] = jnp.where(lane_head == h, k, zero)
            vb_s[row, 0:width] = jnp.where(lane_head == h, v, zero)
            vb_s[row, width:] = jnp.where(lane_head == h, one, zero)
        g_s[at, :] = jax.nn.sigmoid(vg[:, width:] + gb_ref[...])

    repeat(chunks, project)

    def attend(ch):
        at = pl.ds(ch * CHUNK, CHUNK)
        q = q_s[at, :]
        alive = live_row > 0.0
        mate = lax.rem(iota((CHUNK, tokens), 0), local) == lax.rem(iota((CHUNK, tokens), 1), local)
        probs = []
        for h in range(HEAD_COUNT):
            scores = dot_t(q, kb_s[h * tokens : (h + 1) * tokens, :])
            scores = jnp.where(mate, jnp.where(alive, scores, MASKED), OTHER)
            probs.append(
                jnp.exp(scores - jnp.max(scores, axis=-1, keepdims=True)).astype(BF16)
            )
        both = dot(jnp.concatenate(probs, axis=1), vb_s[...])
        attended = both[:, :width] / both[:, width:]
        gated = (attended * g_s[at, :]).astype(BF16)
        update = dot(gated, wo[...]) + ob_ref[...]
        after = token_rows(ch) + update
        revised = after.astype(BF16)
        out_ref[pl.ds(ch * per, per)] = after.reshape(per, local, width).astype(BF16)
        normed = layer_norm(revised.astype(F32), pg_ref[...], pa_ref[...])
        projected = (dot_t(normed, wt_ref[...]) + bt_ref[...]) * live_s[at, :]
        projected = projected.astype(BF16)
        wide = jnp.where(own_seq, dot(projected, spread_e), 0.0).astype(BF16)
        mine = dot(sel, wide)[:local].astype(BF16)
        if chunks == 1:
            rsend[...] = mine
        else:
            rsend[:, pl.ds(pl.multiple_of(ch * ke, ke), ke)] = mine
        if chunks == 1:
            post_right()
        left = dot(perm, projected).astype(BF16)
        for e in range(OUTER_CHANNELS):
            part = dot(left, w2[:, e * PAIR_DIM : (e + 1) * PAIR_DIM]).astype(BF16)
            for i in range(local):
                t_s[ch, e * per : (e + 1) * per, i * PAIR_DIM : (i + 1) * PAIR_DIM] = part[
                    i * per : (i + 1) * per
                ]

    def post_right():
        rbuf[me] = rsend[...]

        def post(k):
            pltpu.make_async_remote_copy(
                src_ref=rsend,
                dst_ref=rbuf.at[me],
                send_sem=ssem2,
                recv_sem=rsem2,
                device_id={"dap": lax.rem(me + k, n)},
                device_id_type=MESH,
            ).start()

        each_peer(n, post)

    repeat(chunks, attend)
    out_copy = pltpu.make_async_copy(out_ref, out_hbm, osem.at[0])
    out_copy.start()
    if chunks > 1:
        post_right()

    pltpu.make_async_copy(rbuf.at[pl.ds(0, n - 1)], rbuf.at[pl.ds(0, n - 1)], rsem2).wait()

    total = None
    for ch in range(chunks):
        right = rbuf[:, :, ch * ke : (ch + 1) * ke].astype(F32).reshape(res, ke).astype(BF16)
        part = dot(right, t_s[ch])
        total = part if total is None else total + part
    inv = inv_s[...]
    for i in range(local):
        pair_ref[i] = (
            total[:, i * PAIR_DIM : (i + 1) * PAIR_DIM] * inv[:, i : i + 1] + cb_ref[...]
        ).astype(BF16)
    pair_copy = pltpu.make_async_copy(pair_ref, pair_hbm, osem.at[1])
    pair_copy.start()
    pltpu.make_async_copy(send.at[pl.ds(0, n - 1)], send.at[pl.ds(0, n - 1)], ssem).wait()
    pltpu.make_async_copy(rbuf.at[pl.ds(0, n - 1)], rbuf.at[pl.ds(0, n - 1)], ssem2).wait()
    out_copy.wait()
    pair_copy.wait()


def shards(n, *args):
    x, occ, flag, ng, na, wqk, wvg, gb, wo, ob, pg, pa, wt, bt, cm, cb = args
    own, res, width = x.shape
    local = res // n
    seqs = occ.shape[0]
    tokens = seqs * local
    chunks = tokens // CHUNK
    ke = OUTER_CHANNELS * (CHUNK // local)
    row = lambda v: v.reshape(1, -1)
    operands = (
        x, occ, row(flag), row(ng), row(na), wqk, wvg, row(gb), wo, row(ob),
        row(pg), row(pa), wt.T, row(bt), cm, row(cb),
    )
    outs = (
        jax.ShapeDtypeStruct((seqs, local, width), BF16),
        jax.ShapeDtypeStruct((local, res, PAIR_DIM), BF16),
    )
    hbm = pl.BlockSpec(memory_space=pl.ANY)
    return pl.pallas_call(
        functools.partial(kernel, n),
        out_shape=outs,
        in_specs=[hbm] * len(operands),
        out_specs=(hbm, hbm),
        scratch_shapes=[
            pltpu.VMEM((n, own * local, width), BF16),
            pltpu.VMEM((n, own * local, width), BF16),
            pltpu.VMEM((local, chunks * ke), BF16),
            pltpu.VMEM((n, local, chunks * ke), BF16),
            pltpu.VMEM(cm.shape, F32),
            pltpu.VMEM((2 * OUTER_CHANNELS, OUTER_CHANNELS * PAIR_DIM), BF16),
            pltpu.VMEM((tokens, width), BF16),
            pltpu.VMEM((HEAD_COUNT * tokens, width), BF16),
            pltpu.VMEM((HEAD_COUNT * tokens, 2 * width), BF16),
            pltpu.VMEM((tokens, width), F32),
            pltpu.VMEM((chunks, ke, local * PAIR_DIM), BF16),
            pltpu.VMEM((res, 8), F32),
            pltpu.VMEM((tokens, 1), F32),
            *[pltpu.VMEM(v.shape, v.dtype) for v in operands + outs],
            pltpu.SemaphoreType.DMA((len(operands),)),
            pltpu.SemaphoreType.DMA((2,)),
            pltpu.SemaphoreType.DMA,
            pltpu.SemaphoreType.DMA,
            pltpu.SemaphoreType.DMA,
            pltpu.SemaphoreType.DMA,
        ],
        compiler_params=pltpu.CompilerParams(
            collective_id=0, has_side_effects=True, vmem_limit_bytes=60 * 1024 * 1024
        ),
        name="evoformer",
    )(*operands)


def solution(mesh):
    in_specs = (P(("grp", "dap"), None, None), P("grp", None), P("grp")) + (P(),) * 13
    out_specs = (P("grp", "dap", None), P(("grp", "dap"), None, None))
    return jax.shard_map(
        functools.partial(shards, mesh.shape["dap"]),
        mesh=mesh, in_specs=in_specs, out_specs=out_specs, check_vma=False,
    )
```

```python
import functools

import jax
import jax.numpy as jnp
from jax import lax
from jax.experimental import pallas as pl
from jax.experimental.pallas import tpu as pltpu
from jax.sharding import PartitionSpec as P

HEAD_COUNT = 8
HEAD_CHANNELS = 32
OUTER_CHANNELS = 32
PAIR_DIM = 128
EPSILON = 1e-05
MASKED = -100000.0
OTHER = -3.0e38
CHUNK = 128

F32 = jnp.float32
BF16 = jnp.bfloat16
MESH = pl.DeviceIdType.MESH


def iota(shape, dim):
    return lax.broadcasted_iota(jnp.int32, shape, dim)


def dot(a, b):
    return jnp.dot(a, b, preferred_element_type=F32)


def dot_t(a, b):
    return lax.dot_general(a, b, (((1,), (1,)), ((), ())), preferred_element_type=F32)


def layer_norm(x, scale, shift):
    centred = x - jnp.mean(x, axis=-1, keepdims=True)
    variance = jnp.mean(centred * centred, axis=-1, keepdims=True)
    return (centred * lax.rsqrt(variance + EPSILON) * scale + shift).astype(BF16)


def repeat(count, body):
    if count == 1:
        body(0)
    else:
        lax.fori_loop(0, count, lambda i, c: (body(i), c)[1], 0)


def each_peer(n, body):
    if n <= 16:
        for k in range(n - 1):
            body(k)
    else:
        lax.fori_loop(0, n - 1, lambda k, c: (body(k), c)[1], 0)


def far_first(me, n, k):
    upper = lax.div(me, n // 2)
    high = n - 1 - k
    high = high - lax.div(me - high + n, n)
    low = k + lax.div(k - me + n, n)
    return upper * low + (1 - upper) * high


def kernel(
    n,
    x_hbm, occ_hbm, flag_hbm, ng_hbm, na_hbm, wqk_hbm, wvg_hbm, gb_hbm, wo_hbm, ob_hbm,
    pg_hbm, pa_hbm, wt_hbm, bt_hbm, cm_hbm, cb_hbm,
    out_hbm, pair_hbm,
    send, recv, rsend, rbuf, cmf, w2,
    q_s, kb_s, vb_s, g_s, t_s, inv_s, live_s,
    x_ref, occ_ref, flag_ref, ng_ref, na_ref, wqk, wvg, gb_ref, wo, ob_ref,
    pg_ref, pa_ref, wt_ref, bt_ref, cm, cb_ref,
    out_ref, pair_ref,
    wsem, osem, ssem, rsem, ssem2, rsem2,
):
    me = lax.axis_index("dap")
    own, res, width = x_hbm.shape
    local = res // n
    seqs = occ_hbm.shape[0]
    tokens = seqs * local
    chunks = tokens // CHUNK
    per = CHUNK // local
    ke = OUTER_CHANNELS * per

    sources = (
        x_hbm, occ_hbm, flag_hbm, cm_hbm, ng_hbm, na_hbm, wqk_hbm, wvg_hbm, gb_hbm, wo_hbm,
        ob_hbm, pg_hbm, pa_hbm, wt_hbm, bt_hbm, cb_hbm,
    )
    targets = (
        x_ref, occ_ref, flag_ref, cm, ng_ref, na_ref, wqk, wvg, gb_ref, wo,
        ob_ref, pg_ref, pa_ref, wt_ref, bt_ref, cb_ref,
    )
    loads = [
        pltpu.make_async_copy(src, dst, wsem.at[i])
        for i, (src, dst) in enumerate(zip(sources, targets))
    ]
    loads[0].start()
    barrier = pltpu.get_barrier_semaphore()

    def greet(k):
        pl.semaphore_signal(
            barrier, inc=1, device_id={"dap": far_first(me, n, k)}, device_id_type=MESH
        )

    each_peer(n, greet)
    for load in loads[1:]:
        load.start()
    loads[0].wait()

    x32 = x_ref[...].astype(F32)
    for p in range(n):
        rows = [x32[s, local * p : local * (p + 1)] for s in range(own)]
        send[p] = jnp.concatenate(rows, axis=0).astype(BF16)
    recv[me] = send[me]

    pl.semaphore_wait(barrier, n - 1)

    def post(k):
        peer = far_first(me, n, k)
        pltpu.make_async_remote_copy(
            src_ref=send.at[peer],
            dst_ref=recv.at[me],
            send_sem=ssem,
            recv_sem=rsem,
            device_id={"dap": peer},
            device_id_type=MESH,
        ).start()

    each_peer(n, post)

    loads[1].wait()
    loads[2].wait()
    occ = occ_ref[...].astype(F32)
    flag = flag_ref[...].astype(F32)
    pick = (iota((8, res), 1) == me * local + iota((8, res), 0)).astype(F32)
    pick = jnp.where(iota((8, res), 0) < local, pick, 0.0)
    live_rs = dot_t(pick, occ) * flag
    owner = (iota((seqs, tokens), 0) == iota((seqs, tokens), 1) // local).astype(F32)
    live_rt = dot(live_rs, owner)
    same = iota((8, tokens), 0) == lax.rem(iota((8, tokens), 1), local)
    live_row = jnp.sum(jnp.where(same, live_rt, 0.0), axis=0, keepdims=True)
    counts = dot(live_rs, occ)
    eye = (iota((res, res), 0) == iota((res, res), 1)).astype(F32)
    counts_t = lax.dot_general(
        eye, counts, (((1,), (1,)), ((), ())),
        precision=lax.Precision.HIGHEST, preferred_element_type=F32,
    )
    inv_s[...] = 1.0 / jnp.maximum(counts_t, 1.0)

    def live_column(ch):
        token = iota((CHUNK, seqs), 0)
        mine = (token // local + ch * per == iota((CHUNK, seqs), 1)).astype(F32) * flag
        spread = dot(mine, occ)
        here = iota((CHUNK, res), 1) == me * local + lax.rem(iota((CHUNK, res), 0), local)
        live_s[pl.ds(ch * CHUNK, CHUNK), :] = jnp.sum(
            jnp.where(here, spread, 0.0), axis=1, keepdims=True
        )

    repeat(chunks, live_column)

    loads[3].wait()
    cmf[...] = cm[...].astype(F32)
    for e in range(OUTER_CHANNELS):
        w2[0:OUTER_CHANNELS, e * PAIR_DIM : (e + 1) * PAIR_DIM] = cmf[
            pl.ds(e, OUTER_CHANNELS, stride=OUTER_CHANNELS), :
        ].astype(BF16)
    w2[OUTER_CHANNELS:, :] = jnp.zeros((OUTER_CHANNELS, OUTER_CHANNELS * PAIR_DIM), BF16)

    spread_e = (
        iota((2 * OUTER_CHANNELS, ke), 0) == OUTER_CHANNELS + iota((2 * OUTER_CHANNELS, ke), 1) // per
    ).astype(BF16)
    own_seq = iota((CHUNK, ke), 0) // local == lax.rem(iota((CHUNK, ke), 1), per)
    sel = (iota((8, CHUNK), 0) == lax.rem(iota((8, CHUNK), 1), local)).astype(BF16)
    perm_row = iota((CHUNK, CHUNK), 0)
    perm = (
        iota((CHUNK, CHUNK), 1) == lax.rem(perm_row, per) * local + perm_row // per
    ).astype(BF16)
    lane_head = iota((CHUNK, width), 1) // HEAD_CHANNELS

    for load in loads[4:]:
        load.wait()
    pltpu.make_async_copy(recv.at[pl.ds(0, n - 1)], recv.at[pl.ds(0, n - 1)], rsem).wait()

    block = own * local
    blocks = CHUNK // block

    def token_rows(ch):
        return recv[pl.ds(ch * blocks, blocks)].astype(F32).reshape(CHUNK, width)

    def project(ch):
        normed = layer_norm(token_rows(ch), ng_ref[...], na_ref[...])
        qk = dot(normed, wqk[...])
        vg = dot(normed, wvg[...])
        at = pl.ds(ch * CHUNK, CHUNK)
        q_s[at, :] = (qk[:, :width] * HEAD_CHANNELS**-0.5).astype(BF16)
        k = qk[:, width:].astype(BF16)
        v = vg[:, :width].astype(BF16)
        zero = jnp.zeros_like(k)
        one = jnp.ones_like(k)
        for h in range(HEAD_COUNT):
            row = pl.ds(h * tokens + ch * CHUNK, CHUNK)
            kb_s[row, :] = jnp.where(lane_head == h, k, zero)
            vb_s[row, 0:width] = jnp.where(lane_head == h, v, zero)
            vb_s[row, width:] = jnp.where(lane_head == h, one, zero)
        g_s[at, :] = jax.nn.sigmoid(vg[:, width:] + gb_ref[...])

    repeat(chunks, project)

    def attend(ch):
        at = pl.ds(ch * CHUNK, CHUNK)
        q = q_s[at, :]
        alive = live_row > 0.0
        mate = lax.rem(iota((CHUNK, tokens), 0), local) == lax.rem(iota((CHUNK, tokens), 1), local)
        probs = []
        for h in range(HEAD_COUNT):
            scores = dot_t(q, kb_s[h * tokens : (h + 1) * tokens, :])
            scores = jnp.where(mate, jnp.where(alive, scores, MASKED), OTHER)
            probs.append(
                jnp.exp(scores - jnp.max(scores, axis=-1, keepdims=True)).astype(BF16)
            )
        both = dot(jnp.concatenate(probs, axis=1), vb_s[...])
        attended = both[:, :width] / both[:, width:]
        gated = (attended * g_s[at, :]).astype(BF16)
        update = dot(gated, wo[...]) + ob_ref[...]
        after = token_rows(ch) + update
        revised = after.astype(BF16)
        out_ref[pl.ds(ch * per, per)] = after.reshape(per, local, width).astype(BF16)
        normed = layer_norm(revised.astype(F32), pg_ref[...], pa_ref[...])
        projected = (dot_t(normed, wt_ref[...]) + bt_ref[...]) * live_s[at, :]
        projected = projected.astype(BF16)
        wide = jnp.where(own_seq, dot(projected, spread_e), 0.0).astype(BF16)
        mine = dot(sel, wide)[:local].astype(BF16)
        if chunks == 1:
            rsend[...] = mine
        else:
            rsend[:, pl.ds(pl.multiple_of(ch * ke, ke), ke)] = mine
        if chunks == 1:
            post_right()
        left = dot(perm, projected).astype(BF16)
        for e in range(OUTER_CHANNELS):
            part = dot(left, w2[:, e * PAIR_DIM : (e + 1) * PAIR_DIM]).astype(BF16)
            for i in range(local):
                t_s[ch, e * per : (e + 1) * per, i * PAIR_DIM : (i + 1) * PAIR_DIM] = part[
                    i * per : (i + 1) * per
                ]

    def post_right():
        rbuf[me] = rsend[...]

        def post(k):
            pltpu.make_async_remote_copy(
                src_ref=rsend,
                dst_ref=rbuf.at[me],
                send_sem=ssem2,
                recv_sem=rsem2,
                device_id={"dap": far_first(me, n, k)},
                device_id_type=MESH,
            ).start()

        each_peer(n, post)

    repeat(chunks, attend)
    out_copy = pltpu.make_async_copy(out_ref, out_hbm, osem.at[0])
    out_copy.start()
    if chunks > 1:
        post_right()

    pltpu.make_async_copy(rbuf.at[pl.ds(0, n - 1)], rbuf.at[pl.ds(0, n - 1)], rsem2).wait()

    total = None
    for ch in range(chunks):
        right = rbuf[:, :, ch * ke : (ch + 1) * ke].astype(F32).reshape(res, ke).astype(BF16)
        part = dot(right, t_s[ch])
        total = part if total is None else total + part
    inv = inv_s[...]
    for i in range(local):
        pair_ref[i] = (
            total[:, i * PAIR_DIM : (i + 1) * PAIR_DIM] * inv[:, i : i + 1] + cb_ref[...]
        ).astype(BF16)
    pair_copy = pltpu.make_async_copy(pair_ref, pair_hbm, osem.at[1])
    pair_copy.start()
    pltpu.make_async_copy(send.at[pl.ds(0, n - 1)], send.at[pl.ds(0, n - 1)], ssem).wait()
    pltpu.make_async_copy(rbuf.at[pl.ds(0, n - 1)], rbuf.at[pl.ds(0, n - 1)], ssem2).wait()
    out_copy.wait()
    pair_copy.wait()


def hand_over(a_ref, b_ref, c_ref, d_ref):
    c_ref[...] = a_ref[...]
    d_ref[...] = b_ref[...]


def shards(n, *args):
    x, occ, flag, ng, na, wqk, wvg, gb, wo, ob, pg, pa, wt, bt, cm, cb = args
    own, res, width = x.shape
    local = res // n
    seqs = occ.shape[0]
    tokens = seqs * local
    chunks = tokens // CHUNK
    ke = OUTER_CHANNELS * (CHUNK // local)
    row = lambda v: v.reshape(1, -1)
    operands = (
        x, occ, row(flag), row(ng), row(na), wqk, wvg, row(gb), wo, row(ob),
        row(pg), row(pa), wt.T, row(bt), cm, row(cb),
    )
    outs = (
        jax.ShapeDtypeStruct((seqs, local, width), BF16),
        jax.ShapeDtypeStruct((local, res, PAIR_DIM), BF16),
    )
    hbm = pl.BlockSpec(memory_space=pl.ANY)
    results = pl.pallas_call(
        functools.partial(kernel, n),
        out_shape=outs,
        in_specs=[hbm] * len(operands),
        out_specs=(hbm, hbm),
        scratch_shapes=[
            pltpu.VMEM((n, own * local, width), BF16),
            pltpu.VMEM((n, own * local, width), BF16),
            pltpu.VMEM((local, chunks * ke), BF16),
            pltpu.VMEM((n, local, chunks * ke), BF16),
            pltpu.VMEM(cm.shape, F32),
            pltpu.VMEM((2 * OUTER_CHANNELS, OUTER_CHANNELS * PAIR_DIM), BF16),
            pltpu.VMEM((tokens, width), BF16),
            pltpu.VMEM((HEAD_COUNT * tokens, width), BF16),
            pltpu.VMEM((HEAD_COUNT * tokens, 2 * width), BF16),
            pltpu.VMEM((tokens, width), F32),
            pltpu.VMEM((chunks, ke, local * PAIR_DIM), BF16),
            pltpu.VMEM((res, 8), F32),
            pltpu.VMEM((tokens, 1), F32),
            *[pltpu.VMEM(v.shape, v.dtype) for v in operands + outs],
            pltpu.SemaphoreType.DMA((len(operands),)),
            pltpu.SemaphoreType.DMA((2,)),
            pltpu.SemaphoreType.DMA,
            pltpu.SemaphoreType.DMA,
            pltpu.SemaphoreType.DMA,
            pltpu.SemaphoreType.DMA,
        ],
        compiler_params=pltpu.CompilerParams(
            collective_id=0, has_side_effects=True, vmem_limit_bytes=60 * 1024 * 1024
        ),
        name="evoformer",
    )(*operands)
    vm = pl.BlockSpec(memory_space=pltpu.VMEM)
    return pl.pallas_call(
        hand_over, out_shape=outs, in_specs=[vm, vm], out_specs=(vm, vm), name="hand_over"
    )(*results)


def solution(mesh):
    in_specs = (P(("grp", "dap"), None, None), P("grp", None), P("grp")) + (P(),) * 13
    out_specs = (P("grp", "dap", None), P(("grp", "dap"), None, None))
    return jax.shard_map(
        functools.partial(shards, mesh.shape["dap"]),
        mesh=mesh, in_specs=in_specs, out_specs=out_specs, check_vma=False,
    )
```
